8 devices in a mesh: rep: 2 (over y, z), dp: 4 (over x, core).
Axes of the slice: x: 2, y: 2, z: 1, core: 2. Of those that a mesh axis runs over, the one named last changes fastest.
Arguments:
- x: bfloat16 [8, 2048, 896], P(('rep', 'dp')), parts along dimension 0
- dy: bfloat16 [8, 2048, 896], P(('rep', 'dp')), parts along dimension 0
- w_gate: bfloat16 [2, 896, 2560], replicated
- w_up: bfloat16 [2, 896, 2560], replicated
- w_down: bfloat16 [2, 2560, 896], replicated
- m_w_gate: float32 [2, 896, 2560], P(None, 'dp')
- m_w_up: float32 [2, 896, 2560], P(None, 'dp')
- m_w_down: float32 [2, 2560, 896], P(None, 'dp')
- v_w_gate: float32 [2, 896, 2560], P(None, 'dp')
- v_w_up: float32 [2, 896, 2560], P(None, 'dp')
- v_w_down: float32 [2, 2560, 896], P(None, 'dp')
Outputs:
- output 1: bfloat16 [4, 896, 2560], P('rep'), parts along dimension 0
- output 2: bfloat16 [4, 896, 2560], P('rep'), parts along dimension 0
- output 3: bfloat16 [4, 2560, 896], P('rep'), parts along dimension 0
- output 4: float32 [4, 896, 2560], P('rep', 'dp'), parts along dimension 0
- output 5: float32 [4, 896, 2560], P('rep', 'dp'), parts along dimension 0
- output 6: float32 [4, 2560, 896], P('rep', 'dp'), parts along dimension 0
- output 7: float32 [4, 896, 2560], P('rep', 'dp'), parts along dimension 0
- output 8: float32 [4, 896, 2560], P('rep', 'dp'), parts along dimension 0
- output 9: float32 [4, 2560, 896], P('rep', 'dp'), parts along dimension 0
There are 2 independent parts. The reference program is written for one: setup_inputs(seed, part) draws one part's arguments, and reference() takes and returns one part's arrays. A program takes and returns all parts, laid end to end along the dimension named above; an argument that names none is the same for every part.
All inputs are finite; a program needn't handle non-finite values.
Results may differ from the reference program's by a relative error of at most 0.022.
Values are sent between devices in bfloat16 or wider.
A program may use at most 2 GiB of HBM per device.

```python
import jax
import jax.numpy as jnp
from jax import lax

SEQUENCES = 4
TOKENS = 2048
D = 896
FF = 2560
LAYERS = 2
NAMES = ("w_gate", "w_up", "w_down")
SHAPES = {"w_gate": (LAYERS, D, FF), "w_up": (LAYERS, D, FF), "w_down": (LAYERS, FF, D)}


def bump(key, n, height):
    away = (jnp.arange(n, dtype=jnp.int32) - jax.random.randint(key, (), 0, n, jnp.int32)) % n
    return jnp.where(away < n // 8, height, 1.0)


def together(key, own, strength):
    shared = jax.random.normal(key, own.shape[1:], jnp.float32)
    return (own + strength * shared) * lax.rsqrt(1 + strength * strength)


def setup_inputs(seed: int = 0, part: int = 0) -> dict:
    kx, kdy, ka, kb, kz, kf, kh, kl, *keys = jax.random.split(jax.random.key(seed), 8 + 3 * len(NAMES))
    kx, kdy, ka, kb = (jax.random.fold_in(k, part) for k in (kx, kdy, ka, kb))
    kw, km, kv = (keys[i::3] for i in range(3))
    shape = (SEQUENCES, TOKENS, D)
    much_x, much_dy = jax.random.uniform(kz, (2,), jnp.float32, 0.0, 1.0)
    loud = 2.0 ** jax.random.uniform(jax.random.fold_in(kz, 1), (), jnp.float32, -1.0, 2.0)
    layers = 2.0 ** jax.random.uniform(kl, (LAYERS, 1, 1), jnp.float32, -1.0, 1.0)
    x = together(ka, jax.random.normal(kx, shape, jnp.float32), much_x) * bump(kf, D, 4.0)
    dy = together(kb, jax.random.normal(kdy, shape, jnp.float32), much_dy)
    drawn = {"x": x.astype(jnp.bfloat16), "dy": (loud * dy * (SEQUENCES * TOKENS) ** -0.5).astype(jnp.bfloat16)}
    for key, name in zip(kw, NAMES, strict=True):
        w = jax.random.normal(key, SHAPES[name], jnp.float32) * SHAPES[name][1] ** -0.5
        drawn[name] = (w * {"w_gate": 1.0, "w_up": bump(kh, FF, 4.0), "w_down": layers}[name]).astype(jnp.bfloat16)
    for key, name in zip(km, NAMES, strict=True):
        drawn[f"m_{name}"] = 0.1 * jax.random.normal(key, SHAPES[name], jnp.float32)
    for key, name in zip(kv, NAMES, strict=True):
        drawn[f"v_{name}"] = jax.random.uniform(key, SHAPES[name], jnp.float32, 0.005, 0.015)
    return drawn


def matmul(a, w):
    return jnp.dot(a, w, preferred_element_type=jnp.float32).astype(jnp.bfloat16)


def normed(h):
    wide = h.astype(jnp.float32)
    scale = lax.rsqrt(jnp.mean(wide**2, -1, keepdims=True) + 1e-6)
    return (wide * scale).astype(jnp.bfloat16)


def layer(h, w):
    a = normed(h)
    gate = jnp.dot(a, w["w_gate"], preferred_element_type=jnp.float32)
    up = jnp.dot(a, w["w_up"], preferred_element_type=jnp.float32)
    return h + matmul((jax.nn.silu(gate) * up).astype(jnp.bfloat16), w["w_down"])


def adamw(w, m, v, g):
    m = 0.9 * m + 0.1 * g
    v = 0.95 * v + 0.05 * g * g
    step = m * lax.rsqrt(v + 1e-8) + 0.1 * w
    return (w - 0.02 * step).astype(jnp.bfloat16), m, v


def stack(weights, h):
    return lax.scan(lambda h, w: (layer(h, w), None), h, weights)[0]


def reference(x, dy, w_gate, w_up, w_down, m_w_gate, m_w_up, m_w_down, v_w_gate, v_w_up, v_w_down):
    weights = dict(zip(NAMES, (w_gate, w_up, w_down), strict=True))

    def take(so_far, sequence):
        h, by_y = sequence
        _, back = jax.vjp(lambda w: stack(w, h), weights)
        return jax.tree.map(lambda total, term: total + term.astype(jnp.float32), so_far, back(by_y)[0]), None

    none_yet = {name: jnp.zeros(w.shape, jnp.float32) for name, w in weights.items()}
    by_weights, _ = lax.scan(take, none_yet, (x, dy))
    gradients = [by_weights[name].astype(jnp.bfloat16).astype(jnp.float32) for name in NAMES]
    new = [
        adamw(w.astype(jnp.float32), m, v, g)
        for w, m, v, g in zip((w_gate, w_up, w_down), (m_w_gate, m_w_up, m_w_down), (v_w_gate, v_w_up, v_w_down), gradients, strict=True)
    ]
    return tuple(one[which] for which in range(3) for one in new)
```

```python
import functools

import jax
import jax.numpy as jnp
from jax import lax
from jax.experimental import pallas as pl
from jax.experimental.pallas import tpu as pltpu

T, D, FF, LAYERS = 2048, 896, 2560, 2
LANES = 128
STRIPES, CHUNKS = 4, 5
CH = STRIPES * LANES
QD, QF = D // 4, FF // 4
TM = 256
TILES = T // TM
PACK = (3, D, LANES)
ANY = pl.BlockSpec(memory_space=pl.ANY)
VMEM = pl.BlockSpec(memory_space=pltpu.VMEM)
BF, F32 = jnp.bfloat16, jnp.float32
TOKEN = jax.ShapeDtypeStruct((8, LANES), F32)
LIMIT = 60 * 1024 * 1024


def shape(*dims, dtype=BF):
    return jax.ShapeDtypeStruct(dims, dtype)


def dot(a, b):
    return jnp.dot(a, b, preferred_element_type=F32)


def dot_nt(a, b):
    return lax.dot_general(a, b, (((1,), (1,)), ((), ())), preferred_element_type=F32)


def sigmoid(g):
    return 0.5 * jnp.tanh(0.5 * g) + 0.5


def scale_of(wide):
    return lax.rsqrt(jnp.mean(wide * wide, -1, keepdims=True) + 1e-6)


def rows(t, size=TM):
    return pl.ds(pl.multiple_of(t * size, size), size)


def params(**kw):
    return pltpu.CompilerParams(vmem_limit_bytes=LIMIT, **kw)


def cost(flops, nbytes):
    return pl.CostEstimate(flops=int(flops), bytes_accessed=int(nbytes), transcendentals=0)


MATMUL = 2 * T * D * FF


def forward_kernel(x_ref, dy_ref, wg_ref, wu_ref, wd_ref, h_out, a_out, at_out, dyt_out, tok, a0, acc, h_v, a_v, at_v, dyt_v, sems):
    j = pl.program_id(0)

    @pl.when(j == 0)
    def _():
        def body(t, _):
            wide = x_ref[0, rows(t), :].astype(F32)
            a0[rows(t), :] = (wide * scale_of(wide)).astype(BF)
            return 0

        lax.fori_loop(0, TILES, body, 0)

    def tile(t, first, last):
        g = dot(a0[rows(t), :], wg_ref[0])
        u = dot(a0[rows(t), :], wu_ref[0])
        z = (g * sigmoid(g) * u).astype(BF)
        part = dot(z, wd_ref[0])
        if first:
            acc[rows(t), :] = part
        elif not last:
            acc[rows(t), :] += part
        else:
            h = x_ref[0, rows(t), :] + (acc[rows(t), :] + part).astype(BF)
            h_v[rows(t), :] = h
            wide = h.astype(F32)
            a = (wide * scale_of(wide)).astype(BF)
            a_v[rows(t), :] = a
            at_v[:, rows(t)] = a.T
            for i, (src, dst) in enumerate(((h_v, h_out), (a_v, a_out))):
                pltpu.make_async_copy(src.at[rows(t)], dst.at[rows(t)], sems.at[i, t]).start()
            pltpu.make_async_copy(at_v.at[:, rows(t)], at_out.at[:, rows(t)], sems.at[2, t]).start()

    @pl.when(j == 0)
    def _():
        lax.fori_loop(0, TILES, lambda t, _: (tile(t, True, False), 0)[1], 0)

    @pl.when((j > 0) & (j < CHUNKS - 1))
    def _():
        lax.fori_loop(0, TILES, lambda t, _: (tile(t, False, False), 0)[1], 0)

    @pl.when(j == 1)
    def _():
        def body(t, _):
            dyt_v[:, rows(t)] = dy_ref[0, rows(t), :].T
            pltpu.make_async_copy(dyt_v.at[:, rows(t)], dyt_out.at[:, rows(t)], sems.at[3, t]).start()
            return 0

        lax.fori_loop(0, TILES, body, 0)

    @pl.when(j == CHUNKS - 1)
    def _():
        lax.fori_loop(0, TILES, lambda t, _: (tile(t, False, True), 0)[1], 0)

        def finish(t, _):
            for i, (src, dst) in enumerate(((h_v, h_out), (a_v, a_out))):
                pltpu.make_async_copy(src.at[rows(t)], dst.at[rows(t)], sems.at[i, t]).wait()
            pltpu.make_async_copy(at_v.at[:, rows(t)], at_out.at[:, rows(t)], sems.at[2, t]).wait()
            pltpu.make_async_copy(dyt_v.at[:, rows(t)], dyt_out.at[:, rows(t)], sems.at[3, t]).wait()
            return 0

        lax.fori_loop(0, TILES, finish, 0)


def forward(x, dy, wg, wu, wd):
    whole = pl.BlockSpec((1, T, D), lambda j: (0, 0, 0), pipeline_mode=pl.Buffered(1))
    return pl.pallas_call(
        forward_kernel,
        grid=(CHUNKS,),
        in_specs=[
            whole,
            whole,
            pl.BlockSpec((1, D, CH), lambda j: (0, 0, j)),
            pl.BlockSpec((1, D, CH), lambda j: (0, 0, j)),
            pl.BlockSpec((1, CH, D), lambda j: (0, j, 0)),
        ],
        out_specs=[ANY] * 5,
        out_shape=[shape(T, D), shape(T, D), shape(D, T), shape(D, T), TOKEN],
        scratch_shapes=[
            pltpu.VMEM((T, D), BF),
            pltpu.VMEM((T, D), F32),
            pltpu.VMEM((T, D), BF),
            pltpu.VMEM((T, D), BF),
            pltpu.VMEM((D, T), BF),
            pltpu.VMEM((D, T), BF),
            pltpu.SemaphoreType.DMA((4, TILES)),
        ],
        compiler_params=params(dimension_semantics=("arbitrary",)),
        cost_estimate=cost(3 * MATMUL, 30e6),
        name="forward_0",
    )(x, dy, wg, wu, wd)


def chunk_kernel(layer, j, keep_d, *refs):
    a_in, at_in, d_in, dt_in, wg_in, wu_in, wd_in = refs[:7]
    refs = refs[8 + (2 if keep_d == 2 else 0) :]
    if keep_d:
        send, keep, dg_out, du_out, tok = refs[:5]
        refs = refs[5:]
    else:
        send, keep, tok = refs[:3]
        refs = refs[3:]
    a, at, d, dt, wg, wu, wd, z, dg, du, both, sems, tile_sems = refs
    me = lax.axis_index("dp")
    chip, core = me // 2, me % 2

    loads = []
    for p in range(STRIPES):
        cols = pl.ds(QF * p + LANES * j, LANES)
        at_p = pl.ds(LANES * p, LANES)
        loads.append((wg_in.at[layer, :, cols], wg.at[:, at_p]))
        loads.append((wu_in.at[layer, :, cols], wu.at[:, at_p]))
        loads.append((wd_in.at[layer, cols, :], wd.at[at_p, :]))
    loads = [pltpu.make_async_copy(s, t, sems.at[i]) for i, (s, t) in enumerate(loads)]
    for copy in loads:
        copy.start()
    tiles = [[pltpu.make_async_copy(s.at[pl.ds(TM * t, TM)], v.at[pl.ds(TM * t, TM)], tile_sems.at[i, t]) for i, (s, v) in enumerate(((a_in, a), (d_in, d)))] for t in range(TILES)]
    for pair in tiles:
        for copy in pair:
            copy.start()
    n = len(loads)
    late = [pltpu.make_async_copy(dt_in, dt, sems.at[n]), pltpu.make_async_copy(at_in, at, sems.at[n + 1])]
    for copy in late:
        copy.start()
    for copy in loads:
        copy.wait()

    def first(t, _):
        for i, (s, v) in enumerate(((a_in, a), (d_in, d))):
            pltpu.make_async_copy(s.at[rows(t)], v.at[rows(t)], tile_sems.at[i, t]).wait()
        g = dot(a[rows(t), :], wg[...])
        u = dot(a[rows(t), :], wu[...])
        dz = dot_nt(d[rows(t), :], wd[...]).astype(BF).astype(F32)
        s = sigmoid(g)
        silu = g * s
        z[rows(t), :] = (silu * u).astype(BF)
        du[rows(t), :] = (dz * silu).astype(BF)
        dg[rows(t), :] = (dz * u * (s + silu * (1 - s))).astype(BF)
        return 0

    lax.fori_loop(0, TILES, first, 0)

    stores = []
    if keep_d:
        for p in range(STRIPES):
            cols = pl.ds(QF * p + LANES * j, LANES)
            at_p = pl.ds(LANES * p, LANES)
            stores.append(pltpu.make_async_copy(dg.at[:, at_p], dg_out.at[:, cols], sems.at[n + 2 + 2 * p]))
            stores.append(pltpu.make_async_copy(du.at[:, at_p], du_out.at[:, cols], sems.at[n + 3 + 2 * p]))
        for copy in stores:
            copy.start()

    def place(q):
        return (q % 2) ^ core, (q // 2) ^ chip

    late[0].wait()

    def down(b0, size):
        r = dot(dt[pl.ds(b0, size), :], z[...])
        for p in range(STRIPES):
            side, rel = place(p)
            for i in range(size // LANES):
                block = r[LANES * i : LANES * (i + 1), LANES * p : LANES * (p + 1)].T.astype(BF)
                both[side, rel, 2, pl.ds(b0 + LANES * i, LANES), :] = block

    lax.fori_loop(0, 3, lambda b, _: (down(pl.multiple_of(b * 256, 256), 256), 0)[1], 0)
    down(768, 128)
    late[1].wait()

    def gate_up(q, _):
        side, rel = place(q)
        for i, grad in enumerate((dg, du)):
            r = dot(at[pl.ds(pl.multiple_of(q * QD, 32), QD), :], grad[...]).astype(BF)
            for p in range(STRIPES):
                both[side, rel, i, QD * p : QD * (p + 1), :] = r[:, LANES * p : LANES * (p + 1)]
        return 0

    lax.fori_loop(0, 4, gate_up, 0)
    k = n + 2 + 2 * STRIPES
    out = [pltpu.make_async_copy(both.at[1], send, sems.at[k]), pltpu.make_async_copy(both.at[0], keep, sems.at[k + 1])]
    for copy in out:
        copy.start()
    for copy in out + stores:
        copy.wait()


def chunk(layer, j, a, at, d, dt, w, tok, kept=None, keep_d=False):
    mode = 0 if not keep_d else (1 if kept is None else 2)
    out_shape = [shape(2, *PACK), shape(2, *PACK)]
    if mode:
        out_shape += [shape(T, FF), shape(T, FF)]
    extra = list(kept) if mode == 2 else []
    return pl.pallas_call(
        functools.partial(chunk_kernel, layer, j, mode),
        in_specs=[ANY] * (8 + len(extra)),
        out_specs=[ANY] * (len(out_shape) + 1),
        out_shape=out_shape + [TOKEN],
        input_output_aliases={8: 2, 9: 3} if mode == 2 else {},
        scratch_shapes=[
            pltpu.VMEM((T, D), BF),
            pltpu.VMEM((D, T), BF),
            pltpu.VMEM((T, D), BF),
            pltpu.VMEM((D, T), BF),
            pltpu.VMEM((D, CH), BF),
            pltpu.VMEM((D, CH), BF),
            pltpu.VMEM((CH, D), BF),
            pltpu.VMEM((T, CH), BF),
            pltpu.VMEM((T, CH), BF),
            pltpu.VMEM((T, CH), BF),
            pltpu.VMEM((2, 2, *PACK), BF),
            pltpu.SemaphoreType.DMA((3 * STRIPES + 4 + 2 * STRIPES,)),
            pltpu.SemaphoreType.DMA((2, TILES)),
        ],
        compiler_params=params(),
        cost_estimate=cost(6 * MATMUL / CHUNKS, 20e6),
        name=f"chunk_{layer}_{j}",
    )(a, at, d, dt, *w, tok, *extra)


def states_kernel(dg, du, wg, wu, h, dy, x, tok_in, dh_out, dht_out, a0_out, a0t_out, tok):
    da = dot_nt(dg[...], wg[0]) + dot_nt(du[...], wu[0])
    da = da.astype(BF).astype(F32)
    wide = h[...].astype(F32)
    s = scale_of(wide)
    along = jnp.sum(da * wide, -1, keepdims=True) * (s * s * s / D)
    dh = dy[0] + (da * s - wide * along).astype(BF)
    dh_out[...] = dh
    dht_out[...] = dh.T
    wide = x[0].astype(F32)
    a0 = (wide * scale_of(wide)).astype(BF)
    a0_out[...] = a0
    a0t_out[...] = a0.T


def states(dg, du, wg, wu, h, dy, x, tok):
    by_row = lambda n: pl.BlockSpec((TM, n), lambda t: (t, 0))
    by_row3 = pl.BlockSpec((1, TM, D), lambda t: (0, t, 0))
    by_col = pl.BlockSpec((D, TM), lambda t: (0, t))
    weight = pl.BlockSpec((1, D, FF), lambda t: (1, 0, 0), pipeline_mode=pl.Buffered(1))
    return pl.pallas_call(
        states_kernel,
        grid=(TILES,),
        in_specs=[by_row(FF), by_row(FF), weight, weight, by_row(D), by_row3, by_row3, ANY],
        out_specs=[by_row(D), by_col, by_row(D), by_col, ANY],
        out_shape=[shape(T, D), shape(D, T), shape(T, D), shape(D, T), TOKEN],
        compiler_params=params(dimension_semantics=("arbitrary",)),
        cost_estimate=cost(2 * MATMUL, 50e6),
        name="states_1",
    )(dg, du, wg, wu, h, dy, x, tok)


def add_kernel(keep, got, tok_in, out, tok):
    out[...] = (keep[0].astype(F32) + got[0].astype(F32)).astype(BF)


def add(keep, got, tok):
    second = pl.BlockSpec((1, *PACK), lambda i: (1, 0, 0, 0))
    return pl.pallas_call(
        add_kernel,
        grid=(1,),
        in_specs=[second, second, ANY],
        out_specs=[pl.BlockSpec(PACK, lambda i: (0, 0, 0)), ANY],
        out_shape=[shape(*PACK), TOKEN],
        compiler_params=params(),
        cost_estimate=cost(2e9, 3e6),
        name="chip_sum",
    )(keep, got, tok)


def blocks(layer, j, owner_rows, owner_hidden):
    for which in range(2):
        for p in range(STRIPES):
            yield which, (layer, owner_rows, pl.ds(QF * p + LANES * j, LANES)), QD * p, QD
    for b in range(D // LANES):
        yield 2, (layer, owner_hidden, pl.ds(LANES * b, LANES)), LANES * b, LANES


def adamw_kernel(layer, j, aliased, *refs):
    keep, got, across = refs[:3]
    w_in, m_in, v_in = refs[3:6], refs[6:9], refs[9:12]
    refs = refs[13 + (6 if aliased else 0) :]
    new_w, m_out, v_out = refs[0], refs[1:4], refs[4:7]
    w, m, v, sems = refs[8:]
    me = lax.axis_index("dp")
    mine = list(blocks(layer, j, pl.ds(0, QD), pl.ds(LANES * j, LANES)))
    whole = list(
        blocks(
            layer,
            j,
            pl.ds(pl.multiple_of(QD * me, 32), QD),
            pl.ds(pl.multiple_of(QF * me + LANES * j, LANES), LANES),
        )
    )
    loads = []
    for i, ((which, at, row, size), (_, at_whole, _, _)) in enumerate(zip(mine, whole)):
        to = (which, pl.ds(row, size))
        loads.append(
            [
                pltpu.make_async_copy(w_in[which].at[at_whole], w.at[to], sems.at[0, i]),
                pltpu.make_async_copy(m_in[which].at[at], m.at[to], sems.at[1, i]),
                pltpu.make_async_copy(v_in[which].at[at], v.at[to], sems.at[2, i]),
            ]
        )
        for copy in loads[-1]:
            copy.start()
    stores = []
    for i, (which, at, row, size) in enumerate(mine):
        for copy in loads[i]:
            copy.wait()
        part = (which, pl.ds(row, size))
        g = keep[0, which, row : row + size].astype(F32) + got[0, which, row : row + size].astype(F32)
        g = (g + across[which, row : row + size].astype(F32)).astype(BF).astype(F32)
        m_new = 0.9 * m[part] + 0.1 * g
        v_new = 0.95 * v[part] + 0.05 * g * g
        wide = w[part].astype(F32)
        step = m_new * lax.rsqrt(v_new + 1e-8) + 0.1 * wide
        new_w[part] = (wide - 0.02 * step).astype(BF)
        m[part] = m_new
        v[part] = v_new
        stores.append(pltpu.make_async_copy(m.at[part], m_out[which].at[at], sems.at[3, i]))
        stores.append(pltpu.make_async_copy(v.at[part], v_out[which].at[at], sems.at[4, i]))
        for copy in stores[-2:]:
            copy.start()
    for copy in stores:
        copy.wait()


def adamw(layer, j, keep, got, across, w, m, v, tok, so_far):
    first = pl.BlockSpec((1, *PACK), lambda i: (0, 0, 0, 0))
    packed = pl.BlockSpec(PACK, lambda i: (0, 0, 0))
    aliased = so_far is not None
    extra = list(so_far) if aliased else []
    n = 3 * STRIPES + D // LANES
    out = pl.pallas_call(
        functools.partial(adamw_kernel, layer, j, aliased),
        grid=(1,),
        in_specs=[first, first, packed] + [ANY] * (10 + len(extra)),
        out_specs=[packed] + [ANY] * 7,
        out_shape=[shape(*PACK)] + [jax.ShapeDtypeStruct(t.shape, t.dtype) for t in (*m, *v)] + [TOKEN],
        input_output_aliases={13 + i: 1 + i for i in range(6)} if aliased else {},
        scratch_shapes=[pltpu.VMEM(PACK, BF), pltpu.VMEM(PACK, F32), pltpu.VMEM(PACK, F32), pltpu.SemaphoreType.DMA((5, n))],
        compiler_params=params(),
        cost_estimate=cost(4e9, 8e6),
        name=f"adamw_{layer}_{j}",
    )(keep, got, across, *w, *m, *v, tok, *extra)
    return out[0], tuple(out[1:7]), out[7]


def place_kernel(layer, j, aliased, *refs):
    parts = refs[:4]
    refs = refs[5 + (3 if aliased else 0) :]
    outs, sems = refs[:3], refs[4]
    me = lax.axis_index("dp")
    chip, core = me // 2, me % 2
    copies = []
    for k, (part, rel_chip, rel_core) in enumerate(zip(parts, (0, 1, 0, 1), (0, 0, 1, 1))):
        q = (chip ^ rel_chip) * 2 + (core ^ rel_core)
        where = blocks(layer, j, pl.ds(pl.multiple_of(QD * q, 32), QD), pl.ds(pl.multiple_of(QF * q + LANES * j, LANES), LANES))
        for i, (which, at, row, size) in enumerate(where):
            copies.append(pltpu.make_async_copy(part.at[which, pl.ds(row, size)], outs[which].at[at], sems.at[k, i]))
            copies[-1].start()
    for copy in copies:
        copy.wait()


def place(layer, j, parts, w, tok, so_far):
    aliased = so_far is not None
    extra = list(so_far) if aliased else []
    n = 2 * STRIPES + D // LANES
    out = pl.pallas_call(
        functools.partial(place_kernel, layer, j, aliased),
        in_specs=[VMEM] * 4 + [ANY] * (1 + len(extra)),
        out_specs=[ANY] * 4,
        out_shape=[jax.ShapeDtypeStruct(t.shape, t.dtype) for t in w] + [TOKEN],
        input_output_aliases={5 + i: i for i in range(3)} if aliased else {},
        scratch_shapes=[pltpu.SemaphoreType.DMA((4, n))],
        compiler_params=params(),
        cost_estimate=cost(2e9, 6e6),
        name=f"place_{layer}_{j}",
    )(*parts, tok, *extra)
    return tuple(out[:3]), out[3]


ORDER = (
    "C10 S10 C11 S11 C12 S12 A10 C13 S13 A11 C14 S14 A12 D A13 C00 S00 A14 P10 C01 S01 P11 C02 S02 A00 P12"
    " C03 S03 A01 P13 C04 S04 A02 P14 A03 P00 A04 P01 P02 P03 P04"
).split()


def solution(mesh):
    from jax.sharding import PartitionSpec as P

    across = [(i, i ^ 2) for i in range(4)]
    partner = [(i, i ^ 1) for i in range(4)]

    def step(x, dy, wg, wu, wd, *moments):
        w, m, v = (wg, wu, wd), moments[:3], moments[3:]
        h, a1, a1t, dyt, tok = forward(x, dy, wg, wu, wd)
        dy2 = dy.reshape(T, D)
        inputs = {1: (a1, a1t, dy2, dyt)}
        kept, mv, new = None, None, None
        keep, got, crossed, parts = {}, {}, {}, {}
        for name in ORDER:
            kind, key = name[0], tuple(int(i) for i in name[1:])
            if kind == "C":
                layer, j = key
                if layer:
                    send, keep[key], *kept, tok = chunk(layer, j, *inputs[layer], w, tok, kept, True)
                else:
                    send, keep[key], tok = chunk(layer, j, *inputs[layer], w, tok)
                got[key] = lax.ppermute(send, "dp", partner)
            elif kind == "S":
                total, tok = add(keep[key], got[key], tok)
                crossed[key] = lax.ppermute(total, "dp", across)
            elif kind == "A":
                own, mv, tok = adamw(*key, keep[key], got[key], crossed[key], w, m, v, tok, mv)
                other = lax.ppermute(own, "dp", across)
                parts[key] = (own, other, lax.ppermute(own, "dp", partner), lax.ppermute(other, "dp", partner))
            elif kind == "P":
                new, tok = place(*key, parts[key], w, tok, new)
            else:
                dh, dht, a0, a0t, tok = states(*kept, wg, wu, h, dy, x, tok)
                inputs[0] = (a0, a0t, dh, dht)
        return (*new, *mv)

    whole, shard = P(), P(None, "dp")
    return jax.shard_map(
        step,
        mesh=mesh,
        in_specs=(P(("rep", "dp")),) * 2 + (whole,) * 3 + (shard,) * 6,
        out_specs=(P("rep"),) * 3 + (P("rep", "dp"),) * 6,
        check_vma=False,
    )
```
